32 devices in a mesh: zero: 2 (over core), tp: 4 (over y, x), site: 4 (over z).
Axes of the slice: x: 2, y: 2, z: 4, core: 2. Of those that a mesh axis runs over, the one named last changes fastest.
Arguments:
- weight_gate: float32 [8192, 8192], P(('site', 'zero'), 'tp'), parts along dimension 0, may hold values from -0.1875 to 0.1875
- moment_gate: float32 [8192, 8192], P(('site', 'zero'), 'tp'), parts along dimension 0, may hold values from -0.125 to 0.125
- square_gate: float32 [8192, 8192], P(('site', 'zero'), 'tp'), parts along dimension 0, may hold values from -0.125 to 0.125
- weight_up: float32 [8192, 8192], P(('site', 'zero'), 'tp'), parts along dimension 0, may hold values from -0.1875 to 0.1875
- moment_up: float32 [8192, 8192], P(('site', 'zero'), 'tp'), parts along dimension 0, may hold values from -0.125 to 0.125
- square_up: float32 [8192, 8192], P(('site', 'zero'), 'tp'), parts along dimension 0, may hold values from -0.125 to 0.125
- norm_train: float32 [8192], P(('site', 'zero', 'tp')), parts along dimension 0, may hold values from 0.25 to 1.75
- norm_step: float32 [8192], P(('site', 'zero', 'tp')), parts along dimension 0, may hold values from -0.3 to 0.3
Outputs:
- ready_gate: bfloat16 [8192, 8192], P('site', 'tp'), parts along dimension 0
- ready_up: bfloat16 [8192, 8192], P('site', 'tp'), parts along dimension 0
- scale_gate: float32 [32768], P(('site', 'tp')), parts along dimension 0
- scale_up: float32 [32768], P(('site', 'tp')), parts along dimension 0
- serve_norm: bfloat16 [8192], P('site'), parts along dimension 0
- latest_gate: float32 [8192, 8192], P(('site', 'zero'), 'tp'), parts along dimension 0
- latest_up: float32 [8192, 8192], P(('site', 'zero'), 'tp'), parts along dimension 0
The draws below stay inside these ranges and needn't reach their ends.
There are 4 independent parts, one for each index of `site`. The reference program is written for one: setup_inputs(seed, part) draws one part's arguments, and reference() takes and returns one part's arrays. A program takes and returns all parts, laid end to end along the dimension named above; each array names one. Nothing has to cross between parts.
All inputs are finite; a program needn't handle non-finite values. Where the reference program divides by a largest or mean magnitude, that divisor is 1e-20 or more.
Results may differ from the reference program's by a relative error of at most 0.001.
Values may be sent and summed in bfloat16 or wider, within the bound.
A program may use at most 192 MiB of HBM per device.

```python
import jax
import jax.numpy as jnp

D_MODEL = 2048
D_INNER = 8192


def with_spikes(values, rng, source, target, shards_of, factor):
    def block_of(dim):
        return (jnp.arange(values.shape[dim]) // (values.shape[dim] // shards_of)).reshape((-1,) + (1,) * (values.ndim - 1 - dim))

    one_side = jax.random.permutation(rng, shards_of)[block_of(target)]
    far = (block_of(target) + shards_of // 2) % shards_of
    return jnp.where((block_of(source) == one_side) | (block_of(source) == far), factor * values, values)


def shard_levels(stream_key, extent, pieces, low, high):
    level = 1.0
    for axis_at, shards_of in pieces:
        steps = jax.random.uniform(jax.random.fold_in(jax.random.fold_in(stream_key, 6), axis_at), (shards_of,), jnp.float32, low / len(pieces), high / len(pieces))
        level = level * jnp.repeat(jnp.exp(steps), extent[axis_at] // shards_of).reshape((-1,) + (1,) * (len(extent) - 1 - axis_at))
    return level


def gaussian(stream_key, shape, spread, reach, shards=(), dtype=jnp.bfloat16):
    values = spread * jax.random.normal(stream_key, shape, jnp.float32)
    if shards:
        values = values * shard_levels(stream_key, shape, shards, -0.22, 0.18)
    return jnp.clip(values, -reach, reach).astype(dtype)


def noise_with(own_key, extent, width, most, cuts, heavy, held_as=jnp.bfloat16):
    values = width * jax.random.normal(own_key, extent, jnp.float32)
    if cuts:
        values = values * shard_levels(own_key, extent, cuts, -0.22, 0.18)
    return jnp.clip(with_spikes(values, jax.random.fold_in(own_key, 3), *heavy), -most, most).astype(held_as)


def setup_inputs(seed: int = 0, part: int = 0) -> dict:
    key_list = jax.random.split(jax.random.key(seed), 9)
    part_splits = jax.random.split(jax.random.fold_in(key_list[8], part), 9)
    return {
        "weight_gate": noise_with(part_splits[0], (D_MODEL, D_INNER), D_MODEL ** -0.5, 0.1875, ((0, 2), (1, 4)), (0, 1, 4, 2.0), jnp.float32),
        "moment_gate": gaussian(part_splits[1], (D_MODEL, D_INNER), D_MODEL ** -0.5, 0.125, ((0, 2), (1, 4)), jnp.float32),
        "square_gate": gaussian(part_splits[2], (D_MODEL, D_INNER), D_MODEL ** -0.5, 0.125, ((0, 2), (1, 4)), jnp.float32),
        "weight_up": noise_with(part_splits[3], (D_MODEL, D_INNER), D_MODEL ** -0.5, 0.1875, ((0, 2), (1, 4)), (0, 1, 4, 2.0), jnp.float32),
        "moment_up": gaussian(part_splits[4], (D_MODEL, D_INNER), D_MODEL ** -0.5, 0.125, ((0, 2), (1, 4)), jnp.float32),
        "square_up": gaussian(part_splits[5], (D_MODEL, D_INNER), D_MODEL ** -0.5, 0.125, ((0, 2), (1, 4)), jnp.float32),
        "norm_train": jnp.clip(1.0 + 0.15 * jax.random.normal(part_splits[6], (D_MODEL,), jnp.float32), 0.25, 1.75),
        "norm_step": jnp.clip(jax.random.uniform(part_splits[7], (D_MODEL,), jnp.float32, -0.3, 0.3) * shard_levels(part_splits[7], (D_MODEL,), ((0, 8),), -0.4, 0.0), -0.3, 0.3),
    }


learn_rate = 0.25
hold_rate = 0.9


def reference(weight_gate, moment_gate, square_gate, weight_up, moment_up, square_up, norm_train, norm_step):
    hold_gate = hold_rate * moment_gate + square_gate
    latest_gate = weight_gate - learn_rate * hold_gate
    hold_up = hold_rate * moment_up + square_up
    latest_up = weight_up - learn_rate * hold_up
    scale_gate = jnp.max(jnp.abs(latest_gate), axis=0)
    ready_gate = (latest_gate / scale_gate).astype(jnp.bfloat16)
    scale_up = jnp.max(jnp.abs(latest_up), axis=0)
    ready_up = (latest_up / scale_up).astype(jnp.bfloat16)
    serve_norm = (norm_train + norm_step).astype(jnp.bfloat16)
    return ready_gate, ready_up, scale_gate, scale_up, serve_norm, latest_gate, latest_up
```

```python
import functools

import jax
import jax.numpy as jnp
from jax import lax
from jax.experimental import pallas as pl
from jax.experimental.pallas import tpu as pltpu
from jax.sharding import PartitionSpec as P

learn_rate = 0.25
hold_rate = 0.9
MESH = pl.DeviceIdType.MESH
SLOTS = 4
CHUNK = 1 << 18
BODY = 1 << 16
SPLIT = 4
NORM_AT = 2
READS = 1
SENDS = 4


def step_kernel(
    n, ntp, wide, height,
    wg, mg, sg, wu, mu, su, nt, ns,
    latest_g, latest_u, ready_g, ready_u, scale_g, scale_u, norm,
    held, peaks, norms, parts, in_sem, part_sem, peak_send, peak_recv, ready_send, ready_recv, norm_send, norm_recv,
):
    rows, columns = wg.shape
    chunks = columns // wide
    steps = 2 * chunks
    tall = rows // READS
    long = rows // SENDS
    group = n * ntp
    zero, tp = lax.axis_index("zero"), lax.axis_index("tp")
    me = zero * ntp + tp
    operands = ((wg, mg, sg), (wu, mu, su))
    latest, ready, scale = (latest_g, latest_u), (ready_g, ready_u), (scale_g, scale_u)

    def reads(s, which, p):
        slot = lax.rem(s, SLOTS)
        at = pl.ds(pl.multiple_of((s // 2) * wide, wide), wide)
        here = pl.ds(pl.multiple_of(p * tall, tall), tall)
        return [
            pltpu.make_async_copy(ref.at[here, at], held.at[slot, k, here], in_sem.at[slot, p, k])
            for k, ref in enumerate(operands[which])
        ]

    def member(d):
        return {"zero": lax.rem(zero + d, n)}

    def other(d):
        to = lax.rem(me + d, group)
        return {"zero": to // ntp, "tp": lax.rem(to, ntp)}

    pieces = [pltpu.make_async_copy(ref, parts.at[k], part_sem.at[k]) for k, ref in enumerate((nt, ns))]
    for copy in pieces:
        copy.start()
    for s in range(min(SLOTS, steps)):
        for p in range(READS):
            for copy in reads(s, s % 2, p):
                copy.start()

    barrier = pltpu.get_barrier_semaphore()

    @pl.loop(1, group)
    def _(d):
        pl.semaphore_signal(barrier, inc=1, device_id=other(d), device_id_type=MESH)


    def norm_copy(d):
        return pltpu.make_async_remote_copy(
            src_ref=norms.at[me], dst_ref=norms.at[me],
            send_sem=norm_send.at[d - 1], recv_sem=norm_recv.at[d - 1],
            device_id=other(d), device_id_type=MESH,
        )

    def send_norm():
        for copy in pieces:
            copy.wait()
        norms[me] = parts[0] + parts[1]

        @pl.loop(1, group)
        def _(d):
            norm_copy(d).start()

    def peak_copy(s, d):
        return pltpu.make_async_remote_copy(
            src_ref=peaks.at[s, zero], dst_ref=peaks.at[s, zero],
            send_sem=peak_send.at[s, d - 1], recv_sem=peak_recv.at[s, d - 1],
            device_id=member(d), device_id_type=MESH,
        )

    def ready_copy(s, which, d, p=None):
        begin, many = (zero * rows, rows) if p is None else (zero * rows + p * long, long)
        block = ready[which].at[
            pl.ds(pl.multiple_of(begin, many), many), pl.ds(pl.multiple_of((s // 2) * wide, wide), wide)
        ]
        return pltpu.make_async_remote_copy(
            src_ref=block, dst_ref=block,
            send_sem=ready_send.at[s, d - 1], recv_sem=ready_recv.at[s, d - 1],
            device_id=member(d), device_id_type=MESH,
        )

    def update(s, which):
        slot = lax.rem(s, SLOTS)
        at = pl.ds(pl.multiple_of((s // 2) * wide, wide), wide)
        def part(i, peak):
            here = pl.ds(pl.multiple_of(i * height, height), height)
            hold = hold_rate * held[slot, 1, here, :] + held[slot, 2, here, :]
            new = held[slot, 0, here, :] - learn_rate * hold
            latest[which][here, at] = new
            return jnp.maximum(peak, jnp.max(jnp.abs(new).reshape(height // 8, 8, wide), axis=0))

        def piece(p, peak):
            for copy in reads(s, which, p):
                copy.wait()
            peak = lax.fori_loop(p * (tall // height), (p + 1) * (tall // height), part, peak)

            @pl.when(s + SLOTS < steps)
            def _():
                for copy in reads(s + SLOTS, which, p):
                    copy.start()

            return peak

        peaks[s, zero] = lax.fori_loop(0, READS, piece, jnp.zeros((8, wide), jnp.float32))


    def finish(s, which):
        at = pl.ds(pl.multiple_of((s // 2) * wide, wide), wide)
        for d in range(1, n):
            peak_copy(s, d).wait_recv()
        peak = peaks[s, 0]
        for k in range(1, n):
            peak = jnp.maximum(peak, peaks[s, k])
        top = jnp.max(peak, axis=0, keepdims=True)
        for k in range(wide // 128):
            scale[which][pl.ds((s // 2) * (wide // 128) + k, 1), :] = top[:, k * 128 : (k + 1) * 128]
        inverse = jnp.broadcast_to(1.0 / top, (8, wide))

        def part(i, carry):
            here = pl.ds(pl.multiple_of(i * height, height), height)
            there = pl.ds(pl.multiple_of(zero * rows + i * height, height), height)
            value = latest[which][here, at].reshape(height // 8, 8, wide) * inverse
            ready[which][there, at] = value.reshape(height, wide).astype(jnp.bfloat16)
            return carry

        def piece(p, carry):
            lax.fori_loop(p * (long // height), (p + 1) * (long // height), part, 0)
            for d in range(1, n):
                ready_copy(s, which, d, p).start()
            return carry

        lax.fori_loop(0, SENDS, piece, 0)

    def tell(s):
        for d in range(1, n):
            peak_copy(s, d).start()

    update(0, 0)

    @pl.loop(0, chunks)
    def _(j):
        update(2 * j + 1, 1)

        @pl.when(j == 0)
        def _():
            pl.semaphore_wait(barrier, group - 1)
            tell(0)

        tell(2 * j + 1)
        finish(2 * j, 0)

        @pl.when(j == min(NORM_AT, chunks - 1))
        def _():
            send_norm()

        @pl.when(j < chunks - 1)
        def _():
            update(2 * j + 2, 0)
            tell(2 * j + 2)

        finish(2 * j + 1, 1)

    @pl.loop(1, group)
    def _(d):
        norm_copy(d).wait()

    lines = nt.shape[0]
    for k in range(group):
        norm[k * lines : (k + 1) * lines, :] = norms[k].astype(jnp.bfloat16)
    @pl.loop(0, chunks)
    def _(j):
        for which in range(2):
            for d in range(1, n):
                peak_copy(2 * j + which, d).wait_send()
                ready_copy(2 * j + which, which, d).wait()


def write_kernel(*refs):
    count = len(refs) // 2
    copies = []
    for k in range(count):
        cuts = SPLIT if refs[k].shape[0] % (16 * SPLIT) == 0 else 1
        each = refs[k].shape[0] // cuts
        for cut in range(cuts):
            at = pl.ds(cut * each, each)
            copies.append(pltpu.make_async_copy(refs[k].at[at], refs[count + k].at[at], refs[-1].at[k, cut]))
    for copy in copies:
        copy.start()
    for copy in copies:
        copy.wait()


def per_device(n, ntp, wg, mg, sg, wu, mu, su, norm_train, norm_step):
    rows, columns = wg.shape
    length = norm_train.shape[0]
    lines = pl.cdiv(length, 128)
    as_lines = lambda x: jnp.pad(x, (0, lines * 128 - length)).reshape(lines, 128)
    wide = min(columns, max(128, CHUNK // rows))
    height = min(rows // max(READS, SENDS), max(16, BODY // wide))
    steps = 2 * (columns // wide)
    group = n * ntp
    f32, bf16 = jnp.float32, jnp.bfloat16
    shapes = [
        ((rows, columns), f32),
        ((rows, columns), f32),
        ((n * rows, columns), bf16),
        ((n * rows, columns), bf16),
        ((columns // 128, 128), f32),
        ((columns // 128, 128), f32),
        ((group * lines, 128), bf16),
    ]
    anywhere = pl.BlockSpec(memory_space=pl.ANY)
    vmem = pl.BlockSpec(memory_space=pltpu.VMEM)
    results = pl.pallas_call(
        functools.partial(step_kernel, n, ntp, wide, height),
        out_shape=[pltpu.VMEM(shape, dtype) for shape, dtype in shapes],
        in_specs=[anywhere] * 6 + [pl.BlockSpec(memory_space=pltpu.HBM)] * 2,
        out_specs=[vmem] * len(shapes),
        scratch_shapes=[
            pltpu.VMEM((SLOTS, 3, rows, wide), f32),
            pltpu.VMEM((steps, n, 8, wide), f32),
            pltpu.VMEM((group, lines, 128), f32),
            pltpu.VMEM((2, lines, 128), f32),
            pltpu.SemaphoreType.DMA((SLOTS, READS, 3)),
            pltpu.SemaphoreType.DMA((2,)),
            pltpu.SemaphoreType.DMA((steps, n - 1)),
            pltpu.SemaphoreType.DMA((steps, n - 1)),
            pltpu.SemaphoreType.DMA((steps, n - 1)),
            pltpu.SemaphoreType.DMA((steps, n - 1)),
            pltpu.SemaphoreType.DMA((group - 1,)),
            pltpu.SemaphoreType.DMA((group - 1,)),
        ],
        compiler_params=pltpu.CompilerParams(
            collective_id=0, has_side_effects=True, vmem_limit_bytes=15 << 20
        ),
        name="step",
    )(wg, mg, sg, wu, mu, su, *(pltpu.with_memory_space_constraint(as_lines(x), pltpu.HBM) for x in (norm_train, norm_step)))
    latest_g, latest_u, ready_g, ready_u, scale_g, scale_u, norm = pl.pallas_call(
        write_kernel,
        out_shape=[jax.ShapeDtypeStruct(shape, dtype) for shape, dtype in shapes],
        in_specs=[vmem] * len(shapes),
        out_specs=[anywhere] * len(shapes),
        scratch_shapes=[pltpu.SemaphoreType.DMA((len(shapes), SPLIT))],
        compiler_params=pltpu.CompilerParams(vmem_limit_bytes=2 << 20),
        name="write",
    )(*results)
    return (
        ready_g, ready_u, scale_g.reshape(columns), scale_u.reshape(columns),
        norm.reshape(group, lines * 128)[:, :length].reshape(group * length), latest_g, latest_u,
    )


def solution(mesh):
    block = P(("site", "zero"), "tp")
    return jax.shard_map(
        functools.partial(per_device, mesh.shape["zero"], mesh.shape["tp"]),
        mesh=mesh,
        in_specs=(block,) * 6 + (P(("site", "zero", "tp")),) * 2,
        out_specs=(
            P("site", "tp"), P("site", "tp"), P(("site", "tp")), P(("site", "tp")), P("site"), block, block,
        ),
        check_vma=False,
    )
```

```python
import functools

import jax
import jax.numpy as jnp
from jax import lax
from jax.experimental import pallas as pl
from jax.experimental.pallas import tpu as pltpu
from jax.sharding import PartitionSpec as P

learn_rate = 0.25
hold_rate = 0.9
MESH = pl.DeviceIdType.MESH
SLOTS = 4
CHUNK = 1 << 18
BODY = 1 << 16
SPLIT = 4
NORM_AT = 2
LATE = 2
READS = 1
SENDS = 4


def step_kernel(
    n, ntp, wide, height, late,
    wg, mg, sg, wu, mu, su, nt, ns,
    latest_g, latest_u, ready_g, ready_u, scale_g, scale_u, norm, sent,
    held, peaks, norms, parts, in_sem, part_sem, peak_send, peak_recv, ready_send, ready_recv, norm_send, norm_recv,
):
    rows, columns = wg.shape
    chunks = columns // wide
    main = chunks - late
    steps = 2 * chunks
    tall = rows // READS
    long = rows // SENDS
    group = n * ntp
    zero, tp = lax.axis_index("zero"), lax.axis_index("tp")
    me = zero * ntp + tp
    operands = ((wg, mg, sg), (wu, mu, su))
    latest, ready, scale = (latest_g, latest_u), (ready_g, ready_u), (scale_g, scale_u)

    def reads(s, which, p):
        slot = lax.rem(s, SLOTS)
        at = pl.ds(pl.multiple_of((s // 2) * wide, wide), wide)
        here = pl.ds(pl.multiple_of(p * tall, tall), tall)
        return [
            pltpu.make_async_copy(ref.at[here, at], held.at[slot, k, here], in_sem.at[slot, p, k])
            for k, ref in enumerate(operands[which])
        ]

    def member(d):
        return {"zero": lax.rem(zero + d, n)}

    def other(d):
        to = lax.rem(me + d, group)
        return {"zero": to // ntp, "tp": lax.rem(to, ntp)}

    pieces = [pltpu.make_async_copy(ref, parts.at[k], part_sem.at[k]) for k, ref in enumerate((nt, ns))]
    for copy in pieces:
        copy.start()
    for s in range(min(SLOTS, steps)):
        for p in range(READS):
            for copy in reads(s, s % 2, p):
                copy.start()

    barrier = pltpu.get_barrier_semaphore()

    @pl.loop(1, group)
    def _(d):
        pl.semaphore_signal(barrier, inc=1, device_id=other(d), device_id_type=MESH)


    def norm_copy(d):
        return pltpu.make_async_remote_copy(
            src_ref=norms.at[me], dst_ref=norms.at[me],
            send_sem=norm_send.at[d - 1], recv_sem=norm_recv.at[d - 1],
            device_id=other(d), device_id_type=MESH,
        )

    def send_norm():
        for copy in pieces:
            copy.wait()
        norms[me] = parts[0] + parts[1]

        @pl.loop(1, group)
        def _(d):
            norm_copy(d).start()

    def peak_copy(s, d):
        return pltpu.make_async_remote_copy(
            src_ref=peaks.at[s, zero], dst_ref=peaks.at[s, zero],
            send_sem=peak_send.at[s, d - 1], recv_sem=peak_recv.at[s, d - 1],
            device_id=member(d), device_id_type=MESH,
        )

    def ready_copy(s, which, d, p=None):
        begin, many = (zero * rows, rows) if p is None else (zero * rows + p * long, long)
        block = ready[which].at[
            pl.ds(pl.multiple_of(begin, many), many), pl.ds(pl.multiple_of((s // 2) * wide, wide), wide)
        ]
        return pltpu.make_async_remote_copy(
            src_ref=block, dst_ref=block,
            send_sem=ready_send.at[s, d - 1], recv_sem=ready_recv.at[s, d - 1],
            device_id=member(d), device_id_type=MESH,
        )

    def update(s, which, t=None):
        slot = lax.rem(s, SLOTS)
        at = pl.ds(pl.multiple_of((s // 2) * wide, wide), wide)
        def part(i, peak):
            here = pl.ds(pl.multiple_of(i * height, height), height)
            hold = hold_rate * held[slot, 1, here, :] + held[slot, 2, here, :]
            new = held[slot, 0, here, :] - learn_rate * hold
            latest[which][here, at] = new
            if t is not None:
                sent[t, here, :] = new
            return jnp.maximum(peak, jnp.max(jnp.abs(new).reshape(height // 8, 8, wide), axis=0))

        def piece(p, peak):
            for copy in reads(s, which, p):
                copy.wait()
            peak = lax.fori_loop(p * (tall // height), (p + 1) * (tall // height), part, peak)

            @pl.when(s + SLOTS < steps)
            def _():
                for copy in reads(s + SLOTS, which, p):
                    copy.start()

            return peak

        peak = lax.fori_loop(0, READS, piece, jnp.zeros((8, wide), jnp.float32))
        if t is None:
            peaks[s, zero] = peak
        else:
            sent[t, rows : rows + 8, :] = peak

    def finish(s, which):
        at = pl.ds(pl.multiple_of((s // 2) * wide, wide), wide)
        for d in range(1, n):
            peak_copy(s, d).wait_recv()
        peak = peaks[s, 0]
        for k in range(1, n):
            peak = jnp.maximum(peak, peaks[s, k])
        top = jnp.max(peak, axis=0, keepdims=True)
        for k in range(wide // 128):
            scale[which][pl.ds((s // 2) * (wide // 128) + k, 1), :] = top[:, k * 128 : (k + 1) * 128]
        inverse = jnp.broadcast_to(1.0 / top, (8, wide))

        def part(i, carry):
            here = pl.ds(pl.multiple_of(i * height, height), height)
            there = pl.ds(pl.multiple_of(zero * rows + i * height, height), height)
            value = latest[which][here, at].reshape(height // 8, 8, wide) * inverse
            ready[which][there, at] = value.reshape(height, wide).astype(jnp.bfloat16)
            return carry

        def piece(p, carry):
            lax.fori_loop(p * (long // height), (p + 1) * (long // height), part, 0)
            for d in range(1, n):
                ready_copy(s, which, d, p).start()
            return carry

        lax.fori_loop(0, SENDS, piece, 0)

    def tell(s):
        for d in range(1, n):
            peak_copy(s, d).start()

    update(0, 0)

    @pl.loop(0, main)
    def _(j):
        update(2 * j + 1, 1)

        @pl.when(j == 0)
        def _():
            pl.semaphore_wait(barrier, group - 1)
            tell(0)

        tell(2 * j + 1)
        finish(2 * j, 0)

        @pl.when(j == min(NORM_AT, main - 1))
        def _():
            send_norm()

        @pl.when(j < main - 1)
        def _():
            update(2 * j + 2, 0)
            tell(2 * j + 2)

        finish(2 * j + 1, 1)

    @pl.loop(0, late)
    def _(j):
        for which in range(2):
            update(2 * (main + j) + which, which, 2 * j + which)

    @pl.loop(1, group)
    def _(d):
        norm_copy(d).wait()

    lines = nt.shape[0]
    for k in range(group):
        norm[k * lines : (k + 1) * lines, :] = norms[k].astype(jnp.bfloat16)
    @pl.loop(0, main)
    def _(j):
        for which in range(2):
            for d in range(1, n):
                peak_copy(2 * j + which, d).wait_send()
                ready_copy(2 * j + which, which, d).wait()


def spread(copies, source, target, sem, cuts):
    each = source.shape[0] // cuts
    for cut in range(cuts):
        at = pl.ds(cut * each, each)
        there = (at, pl.ds(0, source.shape[1]))
        copies.append(pltpu.make_async_copy(source.at[at], target.at[there], sem.at[cut]))


def early_kernel(latest_g, latest_u, ready_g, out_latest_g, out_latest_u, out_ready_g, sem):
    copies = []
    for k, (source, target) in enumerate(((latest_g, out_latest_g), (latest_u, out_latest_u), (ready_g, out_ready_g))):
        spread(copies, source, target, sem.at[k], SPLIT)
    for copy in copies:
        copy.start()
    for copy in copies:
        copy.wait()


def rest_kernel(n, height, ready_u, scale_g, scale_u, norm, sent, *refs):
    others, refs = refs[: n - 1], refs[n - 1 :]
    _, out_ready_g, out_ready_u, out_scale_g, out_scale_u, out_norm, made, tops, sem, more_sem = refs
    count, tall, wide = sent.shape
    rows, width = tall - 8, ready_u.shape[1]
    zero = lax.axis_index("zero")
    copies = []
    spread(copies, ready_u, out_ready_u, sem, SPLIT)
    copies.append(pltpu.make_async_copy(norm, out_norm, more_sem.at[count]))
    for copy in copies:
        copy.start()
    tops[0] = scale_g[...]
    tops[1] = scale_u[...]
    members = (sent, *others)

    for t in range(count):
        peak = sent[t, rows : rows + 8, :]
        for other in others:
            peak = jnp.maximum(peak, other[t, rows : rows + 8, :])
        top = jnp.max(peak, axis=0, keepdims=True)
        at = width + (t // 2) * wide
        for k in range(wide // 128):
            tops[t % 2, pl.ds(at // 128 + k, 1), :] = top[:, k * 128 : (k + 1) * 128]
        inverse = jnp.broadcast_to(1.0 / top, (8, wide))
        for d, member in enumerate(members):
            owner = lax.rem(zero + n - d, n)

            def part(i, carry, t=t, member=member, owner=owner, inverse=inverse):
                here = pl.ds(pl.multiple_of(i * height, height), height)
                there = pl.ds(pl.multiple_of(owner * rows + i * height, height), height)
                value = member[t, here, :].reshape(height // 8, 8, wide) * inverse
                made[t, there, :] = value.reshape(height, wide).astype(jnp.bfloat16)
                return carry

            lax.fori_loop(0, rows // height, part, 0)
        target = (out_ready_g, out_ready_u)[t % 2].at[:, pl.ds(at, wide)]
        copy = pltpu.make_async_copy(made.at[t], target, more_sem.at[t])
        copy.start()
        copies.append(copy)
    for k, target in enumerate((out_scale_g, out_scale_u)):
        copy = pltpu.make_async_copy(tops.at[k], target, more_sem.at[count + 1 + k])
        copy.start()
        copies.append(copy)
    for copy in copies:
        copy.wait()


def per_device(n, ntp, wg, mg, sg, wu, mu, su, norm_train, norm_step):
    rows, columns = wg.shape
    length = norm_train.shape[0]
    lines = pl.cdiv(length, 128)
    as_lines = lambda x: jnp.pad(x, (0, lines * 128 - length)).reshape(lines, 128)
    wide = max(128, min(columns // 4, CHUNK // rows))
    height = min(rows // max(READS, SENDS), max(16, BODY // wide))
    chunks = columns // wide
    late = max(1, chunks * LATE // 8)
    main = chunks - late
    assert main > 0
    steps = 2 * main
    group = n * ntp
    f32, bf16 = jnp.float32, jnp.bfloat16
    dma = pltpu.SemaphoreType.DMA
    shapes = [
        ((rows, columns), f32),
        ((rows, columns), f32),
        ((n * rows, columns), bf16),
        ((n * rows, columns), bf16),
        ((columns // 128, 128), f32),
        ((columns // 128, 128), f32),
        ((group * lines, 128), bf16),
    ]
    between = list(shapes)
    between[2] = between[3] = ((n * rows, main * wide), bf16)
    between.append(((2 * late, rows + 8, wide), f32))
    anywhere = pl.BlockSpec(memory_space=pl.ANY)
    vmem = pl.BlockSpec(memory_space=pltpu.VMEM)
    latest_g, latest_u, ready_g, ready_u, scale_g, scale_u, norm, sent = pl.pallas_call(
        functools.partial(step_kernel, n, ntp, wide, height, late),
        out_shape=[pltpu.VMEM(shape, dtype) for shape, dtype in between],
        in_specs=[anywhere] * 6 + [pl.BlockSpec(memory_space=pltpu.HBM)] * 2,
        out_specs=[vmem] * len(between),
        scratch_shapes=[
            pltpu.VMEM((SLOTS, 3, rows, wide), f32),
            pltpu.VMEM((steps, n, 8, wide), f32),
            pltpu.VMEM((group, lines, 128), f32),
            pltpu.VMEM((2, lines, 128), f32),
            dma((SLOTS, READS, 3)),
            dma((2,)),
            dma((steps, n - 1)),
            dma((steps, n - 1)),
            dma((steps, n - 1)),
            dma((steps, n - 1)),
            dma((group - 1,)),
            dma((group - 1,)),
        ],
        compiler_params=pltpu.CompilerParams(
            collective_id=0, has_side_effects=True, vmem_limit_bytes=14 << 20
        ),
        name="step",
    )(wg, mg, sg, wu, mu, su, *(pltpu.with_memory_space_constraint(as_lines(x), pltpu.HBM) for x in (norm_train, norm_step)))
    others = [lax.ppermute(sent, "zero", [(k, (k + d) % n) for k in range(n)]) for d in range(1, n)]
    costs = lambda size: pl.CostEstimate(flops=0, bytes_accessed=2 * size, transcendentals=0)
    as_out = lambda *k: [jax.ShapeDtypeStruct(*shapes[i]) for i in k]
    latest_g, latest_u, ready_g = pl.pallas_call(
        early_kernel,
        out_shape=as_out(0, 1, 2),
        in_specs=[vmem] * 3,
        out_specs=[anywhere] * 3,
        scratch_shapes=[dma((3, SPLIT))],
        compiler_params=pltpu.CompilerParams(vmem_limit_bytes=1 << 20),
        cost_estimate=costs(12 * rows * columns),
        name="early",
    )(latest_g, latest_u, ready_g)
    ready_g, ready_u, scale_g, scale_u, norm = pl.pallas_call(
        functools.partial(rest_kernel, n, height),
        out_shape=as_out(2, 3, 4, 5, 6),
        in_specs=[vmem] * (5 + n - 1) + [anywhere],
        out_specs=[anywhere] * 5,
        input_output_aliases={5 + n - 1: 0},
        scratch_shapes=[
            pltpu.VMEM((2 * late, n * rows, wide), bf16),
            pltpu.VMEM((2, columns // 128, 128), f32),
            dma((SPLIT,)),
            dma((2 * late + 3,)),
        ],
        compiler_params=pltpu.CompilerParams(vmem_limit_bytes=6 << 20),
        cost_estimate=costs(4 * rows * columns),
        name="rest",
    )(ready_u, scale_g, scale_u, norm, sent, *others, ready_g)
    return (
        ready_g, ready_u, scale_g.reshape(columns), scale_u.reshape(columns),
        norm.reshape(group, lines * 128)[:, :length].reshape(group * length), latest_g, latest_u,
    )


def solution(mesh):
    block = P(("site", "zero"), "tp")
    return jax.shard_map(
        functools.partial(per_device, mesh.shape["zero"], mesh.shape["tp"]),
        mesh=mesh,
        in_specs=(block,) * 6 + (P(("site", "zero", "tp")),) * 2,
        out_specs=(
            P("site", "tp"), P("site", "tp"), P(("site", "tp")), P(("site", "tp")), P("site"), block, block,
        ),
        check_vma=False,
    )
```

```python
import functools

import jax
import jax.numpy as jnp
from jax import lax
from jax.experimental import pallas as pl
from jax.experimental.pallas import tpu as pltpu
from jax.sharding import PartitionSpec as P

learn_rate = 0.25
hold_rate = 0.9
MESH = pl.DeviceIdType.MESH
SLOTS = 4
CHUNK = 1 << 18
BODY = 1 << 17
SPLIT = 4
NORM_AT = 2
LATE = 2
READS = 2
SENDS = 2


def step_kernel(
    n, ntp, wide, height, late,
    wg, mg, sg, wu, mu, su, nt, ns,
    latest_g, latest_u, ready_g, ready_u, scale_g, scale_u, norm, sent,
    held, peaks, norms, parts, in_sem, part_sem, peak_send, peak_recv, ready_send, ready_recv, norm_send, norm_recv,
):
    rows, columns = wg.shape
    chunks = columns // wide
    main = chunks - late
    steps = 2 * chunks
    tall = rows // READS
    long = rows // SENDS
    group = n * ntp
    zero, tp = lax.axis_index("zero"), lax.axis_index("tp")
    me = zero * ntp + tp
    operands = ((wg, mg, sg), (wu, mu, su))
    latest, ready, scale = (latest_g, latest_u), (ready_g, ready_u), (scale_g, scale_u)

    def reads(s, which, p):
        slot = lax.rem(s, SLOTS)
        at = pl.ds(pl.multiple_of((s // 2) * wide, wide), wide)
        here = pl.ds(pl.multiple_of(p * tall, tall), tall)
        return [
            pltpu.make_async_copy(ref.at[here, at], held.at[slot, k, here], in_sem.at[slot, p])
            for k, ref in enumerate(operands[which])
        ]

    def member(d):
        return {"zero": lax.rem(zero + d, n)}

    def other(d):
        to = lax.rem(me + d, group)
        return {"zero": to // ntp, "tp": lax.rem(to, ntp)}

    pieces = [pltpu.make_async_copy(ref, parts.at[k], part_sem.at[k]) for k, ref in enumerate((nt, ns))]
    for copy in pieces:
        copy.start()
    for s in range(min(SLOTS, steps)):
        for p in range(READS):
            for copy in reads(s, s % 2, p):
                copy.start()

    barrier = pltpu.get_barrier_semaphore()

    @pl.loop(1, group)
    def _(d):
        pl.semaphore_signal(barrier, inc=1, device_id=other(d), device_id_type=MESH)


    def norm_copy(d, at):
        return pltpu.make_async_remote_copy(
            src_ref=norms.at[at], dst_ref=norms.at[at], send_sem=norm_send, recv_sem=norm_recv,
            device_id=other(d), device_id_type=MESH,
        )

    def send_norm():
        for copy in pieces:
            copy.wait()
        norms[me] = parts[0] + parts[1]

        @pl.loop(1, group)
        def _(d):
            norm_copy(d, me).start()

    def peak_copy(s, d):
        return pltpu.make_async_remote_copy(
            src_ref=peaks.at[s, zero], dst_ref=peaks.at[s, zero],
            send_sem=peak_send.at[d - 1], recv_sem=peak_recv.at[s, d - 1],
            device_id=member(d), device_id_type=MESH,
        )

    def ready_copy(s, which, d, p=None):
        begin, many = (zero * rows, rows) if p is None else (zero * rows + p * long, long)
        block = ready[which].at[
            pl.ds(pl.multiple_of(begin, many), many), pl.ds(pl.multiple_of((s // 2) * wide, wide), wide)
        ]
        return pltpu.make_async_remote_copy(
            src_ref=block, dst_ref=block,
            send_sem=ready_send.at[which, d - 1], recv_sem=ready_recv.at[which, d - 1],
            device_id=member(d), device_id_type=MESH,
        )

    def update(s, which, t=None):
        slot = lax.rem(s, SLOTS)
        at = pl.ds(pl.multiple_of((s // 2) * wide, wide), wide)
        def part(i, peak):
            here = pl.ds(pl.multiple_of(i * height, height), height)
            hold = hold_rate * held[slot, 1, here, :] + held[slot, 2, here, :]
            new = held[slot, 0, here, :] - learn_rate * hold
            latest[which][here, at] = new
            if t is not None:
                sent[t, here, :] = new
            return jnp.maximum(peak, jnp.max(jnp.abs(new).reshape(height // 8, 8, wide), axis=0))

        def piece(p, peak):
            landed = held.at[slot, :, pl.ds(pl.multiple_of(p * tall, tall), tall)]
            pltpu.make_async_copy(landed, landed, in_sem.at[slot, p]).wait()
            peak = lax.fori_loop(p * (tall // height), (p + 1) * (tall // height), part, peak)

            @pl.when(s + SLOTS < steps)
            def _():
                for copy in reads(s + SLOTS, which, p):
                    copy.start()

            return peak

        peak = lax.fori_loop(0, READS, piece, jnp.zeros((8, wide), jnp.float32))
        if t is None:
            peaks[s, zero] = peak
        else:
            sent[t, rows : rows + 8, :] = peak

    def finish(s, which):
        at = pl.ds(pl.multiple_of((s // 2) * wide, wide), wide)
        for d in range(1, n):
            peak_copy(s, d).wait_recv()
        peak = peaks[s, 0]
        for k in range(1, n):
            peak = jnp.maximum(peak, peaks[s, k])
        top = jnp.max(peak, axis=0, keepdims=True)
        for k in range(wide // 128):
            scale[which][pl.ds((s // 2) * (wide // 128) + k, 1), :] = top[:, k * 128 : (k + 1) * 128]
        inverse = jnp.broadcast_to(1.0 / top, (8, wide))

        def part(i, carry):
            here = pl.ds(pl.multiple_of(i * height, height), height)
            there = pl.ds(pl.multiple_of(zero * rows + i * height, height), height)
            value = latest[which][here, at].reshape(height // 8, 8, wide) * inverse
            ready[which][there, at] = value.reshape(height, wide).astype(jnp.bfloat16)
            return carry

        def piece(p, carry):
            lax.fori_loop(p * (long // height), (p + 1) * (long // height), part, 0)
            for d in range(1, n):
                ready_copy(s, which, d, p).start()
            return carry

        lax.fori_loop(0, SENDS, piece, 0)

    def tell(s):
        for d in range(1, n):
            peak_copy(s, d).start()

    update(0, 0)

    @pl.loop(0, main)
    def _(j):
        update(2 * j + 1, 1)

        @pl.when(j == 0)
        def _():
            pl.semaphore_wait(barrier, group - 1)
            tell(0)

        tell(2 * j + 1)
        finish(2 * j, 0)

        @pl.when(j == min(NORM_AT, main - 1))
        def _():
            send_norm()

        @pl.when(j < main - 1)
        def _():
            update(2 * j + 2, 0)
            tell(2 * j + 2)

        finish(2 * j + 1, 1)

    def close():
        norm_copy(1, pl.ds(0, group - 1)).wait()

        lines = nt.shape[0]
        for k in range(group):
            norm[k * lines : (k + 1) * lines, :] = norms[k].astype(jnp.bfloat16)


    @pl.loop(0, late)
    def _(j):
        update(2 * (main + j), 0, 2 * j)
        pl.when(j == late - 1)(close)
        update(2 * (main + j) + 1, 1, 2 * j + 1)

    for d in range(1, n):
        told = peaks.at[:, zero]
        pltpu.make_async_remote_copy(
            src_ref=told, dst_ref=told, send_sem=peak_send.at[d - 1], recv_sem=peak_recv.at[0, d - 1],
            device_id=member(d), device_id_type=MESH,
        ).wait_send()
        for which in range(2):
            block = ready[which].at[pl.ds(pl.multiple_of(zero * rows, rows), rows)]
            pltpu.make_async_remote_copy(
                src_ref=block, dst_ref=block,
                send_sem=ready_send.at[which, d - 1], recv_sem=ready_recv.at[which, d - 1],
                device_id=member(d), device_id_type=MESH,
            ).wait()


def spread(source, target, sem):
    width = pl.ds(0, source.shape[1])
    each = source.shape[0] // SPLIT
    for cut in range(SPLIT):
        at = pl.ds(cut * each, each)
        pltpu.make_async_copy(source.at[at], target.at[at, width], sem).start()
    return pltpu.make_async_copy(source, target.at[:, width], sem)


def early_kernel(latest_g, latest_u, ready_g, out_latest_g, out_latest_u, out_ready_g, sem):
    copies = []
    for k, (source, target) in enumerate(((latest_g, out_latest_g), (latest_u, out_latest_u), (ready_g, out_ready_g))):
        copies.append(spread(source, target, sem.at[k]))
    for copy in copies:
        copy.wait()


def rest_kernel(n, height, ready_u, scale_g, scale_u, norm, sent, *refs):
    others, refs = refs[: n - 1], refs[n - 1 :]
    _, out_ready_g, out_ready_u, out_scale_g, out_scale_u, out_norm, made, tops, sem, more_sem = refs
    count, tall, wide = sent.shape
    rows, width = tall - 8, ready_u.shape[1]
    zero = lax.axis_index("zero")
    copies = [spread(ready_u, out_ready_u, sem), pltpu.make_async_copy(norm, out_norm, more_sem.at[count])]
    copies[1].start()
    tops[0] = scale_g[...]
    tops[1] = scale_u[...]
    members = (sent, *others)

    for t in range(count):
        peak = sent[t, rows : rows + 8, :]
        for other in others:
            peak = jnp.maximum(peak, other[t, rows : rows + 8, :])
        top = jnp.max(peak, axis=0, keepdims=True)
        at = width + (t // 2) * wide
        for k in range(wide // 128):
            tops[t % 2, pl.ds(at // 128 + k, 1), :] = top[:, k * 128 : (k + 1) * 128]
        inverse = jnp.broadcast_to(1.0 / top, (8, wide))
        for d, member in enumerate(members):
            owner = lax.rem(zero + n - d, n)

            def part(i, carry, t=t, member=member, owner=owner, inverse=inverse):
                here = pl.ds(pl.multiple_of(i * height, height), height)
                there = pl.ds(pl.multiple_of(owner * rows + i * height, height), height)
                value = member[t, here, :].reshape(height // 8, 8, wide) * inverse
                made[t, there, :] = value.reshape(height, wide).astype(jnp.bfloat16)
                return carry

            lax.fori_loop(0, rows // height, part, 0)
        target = (out_ready_g, out_ready_u)[t % 2].at[:, pl.ds(at, wide)]
        copy = pltpu.make_async_copy(made.at[t], target, more_sem.at[t])
        copy.start()
        copies.append(copy)
    for k, target in enumerate((out_scale_g, out_scale_u)):
        copy = pltpu.make_async_copy(tops.at[k], target, more_sem.at[count + 1 + k])
        copy.start()
        copies.append(copy)
    for copy in copies:
        copy.wait()


def per_device(n, ntp, wg, mg, sg, wu, mu, su, norm_train, norm_step):
    rows, columns = wg.shape
    length = norm_train.shape[0]
    lines = pl.cdiv(length, 128)
    as_lines = lambda x: jnp.pad(x, (0, lines * 128 - length)).reshape(lines, 128)
    wide = max(128, min(columns // 4, CHUNK // rows))
    height = min(rows // max(READS, SENDS), max(16, BODY // wide))
    chunks = columns // wide
    late = max(1, chunks * LATE // 8)
    main = chunks - late
    assert main > 0
    steps = 2 * main
    group = n * ntp
    f32, bf16 = jnp.float32, jnp.bfloat16
    dma = pltpu.SemaphoreType.DMA
    shapes = [
        ((rows, columns), f32),
        ((rows, columns), f32),
        ((n * rows, columns), bf16),
        ((n * rows, columns), bf16),
        ((columns // 128, 128), f32),
        ((columns // 128, 128), f32),
        ((group * lines, 128), bf16),
    ]
    between = list(shapes)
    between[2] = between[3] = ((n * rows, main * wide), bf16)
    between.append(((2 * late, rows + 8, wide), f32))
    anywhere = pl.BlockSpec(memory_space=pl.ANY)
    vmem = pl.BlockSpec(memory_space=pltpu.VMEM)
    latest_g, latest_u, ready_g, ready_u, scale_g, scale_u, norm, sent = pl.pallas_call(
        functools.partial(step_kernel, n, ntp, wide, height, late),
        out_shape=[pltpu.VMEM(shape, dtype) for shape, dtype in between],
        in_specs=[anywhere] * 6 + [pl.BlockSpec(memory_space=pltpu.HBM)] * 2,
        out_specs=[vmem] * len(between),
        scratch_shapes=[
            pltpu.VMEM((SLOTS, 3, rows, wide), f32),
            pltpu.VMEM((steps, n, 8, wide), f32),
            pltpu.VMEM((group, lines, 128), f32),
            pltpu.VMEM((2, lines, 128), f32),
            dma((SLOTS, READS)),
            dma((2,)),
            dma((n - 1,)),
            dma((steps, n - 1)),
            dma((2, n - 1)),
            dma((2, n - 1)),
            dma,
            dma,
        ],
        compiler_params=pltpu.CompilerParams(
            collective_id=0, has_side_effects=True, vmem_limit_bytes=14 << 20
        ),
        name="step",
    )(wg, mg, sg, wu, mu, su, *(pltpu.with_memory_space_constraint(as_lines(x), pltpu.HBM) for x in (norm_train, norm_step)))
    others = [lax.ppermute(sent, "zero", [(k, (k + d) % n) for k in range(n)]) for d in range(1, n)]
    costs = lambda size: pl.CostEstimate(flops=0, bytes_accessed=2 * size, transcendentals=0)
    as_out = lambda *k: [jax.ShapeDtypeStruct(*shapes[i]) for i in k]
    latest_g, latest_u, ready_g = pl.pallas_call(
        early_kernel,
        out_shape=as_out(0, 1, 2),
        in_specs=[vmem] * 3,
        out_specs=[anywhere] * 3,
        scratch_shapes=[dma((3,))],
        compiler_params=pltpu.CompilerParams(vmem_limit_bytes=1 << 20),
        cost_estimate=costs(12 * rows * columns),
        name="early",
    )(latest_g, latest_u, ready_g)
    ready_g, ready_u, scale_g, scale_u, norm = pl.pallas_call(
        functools.partial(rest_kernel, n, height),
        out_shape=as_out(2, 3, 4, 5, 6),
        in_specs=[vmem] * (5 + n - 1) + [anywhere],
        out_specs=[anywhere] * 5,
        input_output_aliases={5 + n - 1: 0},
        scratch_shapes=[
            pltpu.VMEM((2 * late, n * rows, wide), bf16),
            pltpu.VMEM((2, columns // 128, 128), f32),
            dma,
            dma((2 * late + 3,)),
        ],
        compiler_params=pltpu.CompilerParams(vmem_limit_bytes=6 << 20),
        cost_estimate=costs(4 * rows * columns),
        name="rest",
    )(ready_u, scale_g, scale_u, norm, sent, *others, ready_g)
    return (
        ready_g, ready_u, scale_g.reshape(columns), scale_u.reshape(columns),
        norm.reshape(group, lines * 128)[:, :length].reshape(group * length), latest_g, latest_u,
    )


def solution(mesh):
    block = P(("site", "zero"), "tp")
    return jax.shard_map(
        functools.partial(per_device, mesh.shape["zero"], mesh.shape["tp"]),
        mesh=mesh,
        in_specs=(block,) * 6 + (P(("site", "zero", "tp")),) * 2,
        out_specs=(
            P("site", "tp"), P("site", "tp"), P(("site", "tp")), P(("site", "tp")), P("site"), block, block,
        ),
        check_vma=False,
    )
```

```python
import functools

import jax
import jax.numpy as jnp
from jax import lax
from jax.experimental import pallas as pl
from jax.experimental.pallas import tpu as pltpu
from jax.sharding import PartitionSpec as P

learn_rate = 0.25
hold_rate = 0.9
MESH = pl.DeviceIdType.MESH
SLOTS = 4
CHUNK = 1 << 18
BODY = 1 << 17
SPLIT = 4
NORM_AT = 2
LATE = 2
READS = 2
RING = 4
SENDS = 2


def step_kernel(
    n, ntp, wide, height, late,
    wg, mg, sg, wu, mu, su, nt, ns,
    latest_g, latest_u, ready_g, ready_u, scale_g, scale_u, norm, sent,
    held, peaks, norms, parts, in_sem, part_sem, peak_send, peak_recv, ready_send, ready_recv, norm_send, norm_recv,
):
    rows, columns = wg.shape
    chunks = columns // wide
    main = chunks - late
    steps = 2 * chunks
    tall = rows // READS
    long = rows // SENDS
    group = n * ntp
    zero, tp = lax.axis_index("zero"), lax.axis_index("tp")
    me = zero * ntp + tp
    operands = ((wg, mg, sg), (wu, mu, su))
    latest, ready, scale = (latest_g, latest_u), (ready_g, ready_u), (scale_g, scale_u)

    def reads(s, which, p):
        slot = lax.rem(s, SLOTS)
        at = pl.ds(pl.multiple_of((s // 2) * wide, wide), wide)
        here = pl.ds(pl.multiple_of(p * tall, tall), tall)
        return [
            pltpu.make_async_copy(ref.at[here, at], held.at[slot, k, here], in_sem.at[slot, p])
            for k, ref in enumerate(operands[which])
        ]

    def member(d):
        return {"zero": lax.rem(zero + d, n)}

    def other(d):
        to = lax.rem(me + d, group)
        return {"zero": to // ntp, "tp": lax.rem(to, ntp)}

    pieces = [pltpu.make_async_copy(ref, parts.at[k], part_sem) for k, ref in enumerate((nt, ns))]
    for copy in pieces:
        copy.start()
    for s in range(min(SLOTS, steps)):
        for p in range(READS):
            for copy in reads(s, s % 2, p):
                copy.start()

    barrier = pltpu.get_barrier_semaphore()

    @pl.loop(1, group)
    def _(d):
        pl.semaphore_signal(barrier, inc=1, device_id=other(d), device_id_type=MESH)


    def norm_copy(d, at):
        return pltpu.make_async_remote_copy(
            src_ref=norms.at[at], dst_ref=norms.at[at], send_sem=norm_send, recv_sem=norm_recv,
            device_id=other(d), device_id_type=MESH,
        )

    def send_norm():
        pltpu.make_async_copy(parts, parts, part_sem).wait()
        norms[me] = parts[0] + parts[1]

        @pl.loop(1, group)
        def _(d):
            norm_copy(d, me).start()

    def peak_copy(s, d):
        return pltpu.make_async_remote_copy(
            src_ref=peaks.at[s, zero], dst_ref=peaks.at[s, zero],
            send_sem=peak_send.at[d - 1], recv_sem=peak_recv.at[lax.rem(s, RING), d - 1],
            device_id=member(d), device_id_type=MESH,
        )

    def ready_copy(s, which, d, p=None):
        begin, many = (zero * rows, rows) if p is None else (zero * rows + p * long, long)
        block = ready[which].at[
            pl.ds(pl.multiple_of(begin, many), many), pl.ds(pl.multiple_of((s // 2) * wide, wide), wide)
        ]
        return pltpu.make_async_remote_copy(
            src_ref=block, dst_ref=block,
            send_sem=ready_send.at[which, d - 1], recv_sem=ready_recv.at[which, d - 1],
            device_id=member(d), device_id_type=MESH,
        )

    def update(s, which, t=None):
        slot = lax.rem(s, SLOTS)
        at = pl.ds(pl.multiple_of((s // 2) * wide, wide), wide)
        def part(i, peak):
            here = pl.ds(pl.multiple_of(i * height, height), height)
            hold = hold_rate * held[slot, 1, here, :] + held[slot, 2, here, :]
            new = held[slot, 0, here, :] - learn_rate * hold
            latest[which][here, at] = new
            if t is not None:
                sent[t, here, :] = new
            return jnp.maximum(peak, jnp.max(jnp.abs(new).reshape(height // 8, 8, wide), axis=0))

        def piece(p, peak):
            landed = held.at[slot, :, pl.ds(pl.multiple_of(p * tall, tall), tall)]
            pltpu.make_async_copy(landed, landed, in_sem.at[slot, p]).wait()
            peak = lax.fori_loop(p * (tall // height), (p + 1) * (tall // height), part, peak)

            @pl.when(s + SLOTS < steps)
            def _():
                for copy in reads(s + SLOTS, which, p):
                    copy.start()

            return peak

        peak = lax.fori_loop(0, READS, piece, jnp.zeros((8, wide), jnp.float32))
        if t is None:
            peaks[s, zero] = peak
        else:
            sent[t, rows : rows + 8, :] = peak

    def finish(s, which):
        at = pl.ds(pl.multiple_of((s // 2) * wide, wide), wide)
        for d in range(1, n):
            peak_copy(s, d).wait_recv()
        peak = peaks[s, 0]
        for k in range(1, n):
            peak = jnp.maximum(peak, peaks[s, k])
        top = jnp.max(peak, axis=0, keepdims=True)
        for k in range(wide // 128):
            scale[which][pl.ds((s // 2) * (wide // 128) + k, 1), :] = top[:, k * 128 : (k + 1) * 128]
        inverse = jnp.broadcast_to(1.0 / top, (8, wide))

        def part(i, carry):
            here = pl.ds(pl.multiple_of(i * height, height), height)
            there = pl.ds(pl.multiple_of(zero * rows + i * height, height), height)
            value = latest[which][here, at].reshape(height // 8, 8, wide) * inverse
            ready[which][there, at] = value.reshape(height, wide).astype(jnp.bfloat16)
            return carry

        def piece(p, carry):
            lax.fori_loop(p * (long // height), (p + 1) * (long // height), part, 0)
            for d in range(1, n):
                ready_copy(s, which, d, p).start()
            return carry

        lax.fori_loop(0, SENDS, piece, 0)

    def tell(s):
        for d in range(1, n):
            peak_copy(s, d).start()

    update(0, 0)

    @pl.loop(0, main)
    def _(j):
        update(2 * j + 1, 1)

        @pl.when(j == 0)
        def _():
            pl.semaphore_wait(barrier, group - 1)
            tell(0)

        tell(2 * j + 1)
        finish(2 * j, 0)

        @pl.when(j == min(NORM_AT, main - 1))
        def _():
            send_norm()

        @pl.when(j < main - 1)
        def _():
            update(2 * j + 2, 0)
            tell(2 * j + 2)

        finish(2 * j + 1, 1)

    def close():
        norm_copy(1, pl.ds(0, group - 1)).wait()

        lines = nt.shape[0]
        for k in range(group):
            norm[k * lines : (k + 1) * lines, :] = norms[k].astype(jnp.bfloat16)


    @pl.loop(0, late)
    def _(j):
        update(2 * (main + j), 0, 2 * j)
        pl.when(j == late - 1)(close)
        update(2 * (main + j) + 1, 1, 2 * j + 1)

    for d in range(1, n):
        told = peaks.at[:, zero]
        pltpu.make_async_remote_copy(
            src_ref=told, dst_ref=told, send_sem=peak_send.at[d - 1], recv_sem=peak_recv.at[0, d - 1],
            device_id=member(d), device_id_type=MESH,
        ).wait_send()
        for which in range(2):
            block = ready[which].at[pl.ds(pl.multiple_of(zero * rows, rows), rows)]
            pltpu.make_async_remote_copy(
                src_ref=block, dst_ref=block,
                send_sem=ready_send.at[which, d - 1], recv_sem=ready_recv.at[which, d - 1],
                device_id=member(d), device_id_type=MESH,
            ).wait()


def spread(source, target, sem):
    width = pl.ds(0, source.shape[1])
    each = source.shape[0] // SPLIT
    for cut in range(SPLIT):
        at = pl.ds(cut * each, each)
        pltpu.make_async_copy(source.at[at], target.at[at, width], sem).start()
    return pltpu.make_async_copy(source, target.at[:, width], sem)


def early_kernel(latest_g, latest_u, ready_g, out_latest_g, out_latest_u, out_ready_g, sem):
    copies = []
    for k, (source, target) in enumerate(((latest_g, out_latest_g), (latest_u, out_latest_u), (ready_g, out_ready_g))):
        copies.append(spread(source, target, sem.at[k]))
    for copy in copies:
        copy.wait()


def rest_kernel(n, height, ready_u, scale_g, scale_u, norm, sent, *refs):
    others, refs = refs[: n - 1], refs[n - 1 :]
    _, out_ready_g, out_ready_u, out_scale_g, out_scale_u, out_norm, made, tops, sem, more_sem = refs
    count, tall, wide = sent.shape
    rows, width = tall - 8, ready_u.shape[1]
    zero = lax.axis_index("zero")
    copies = [spread(ready_u, out_ready_u, sem), pltpu.make_async_copy(norm, out_norm, more_sem.at[count])]
    copies[1].start()
    tops[0] = scale_g[...]
    tops[1] = scale_u[...]
    members = (sent, *others)

    for t in range(count):
        peak = sent[t, rows : rows + 8, :]
        for other in others:
            peak = jnp.maximum(peak, other[t, rows : rows + 8, :])
        top = jnp.max(peak, axis=0, keepdims=True)
        at = width + (t // 2) * wide
        for k in range(wide // 128):
            tops[t % 2, pl.ds(at // 128 + k, 1), :] = top[:, k * 128 : (k + 1) * 128]
        inverse = jnp.broadcast_to(1.0 / top, (8, wide))
        for d, member in enumerate(members):
            owner = lax.rem(zero + n - d, n)

            def part(i, carry, t=t, member=member, owner=owner, inverse=inverse):
                here = pl.ds(pl.multiple_of(i * height, height), height)
                there = pl.ds(pl.multiple_of(owner * rows + i * height, height), height)
                value = member[t, here, :].reshape(height // 8, 8, wide) * inverse
                made[t, there, :] = value.reshape(height, wide).astype(jnp.bfloat16)
                return carry

            lax.fori_loop(0, rows // height, part, 0)
        target = (out_ready_g, out_ready_u)[t % 2].at[:, pl.ds(at, wide)]
        copy = pltpu.make_async_copy(made.at[t], target, more_sem.at[t])
        copy.start()
        copies.append(copy)
    for k, target in enumerate((out_scale_g, out_scale_u)):
        copy = pltpu.make_async_copy(tops.at[k], target, more_sem.at[count + 1 + k])
        copy.start()
        copies.append(copy)
    for copy in copies:
        copy.wait()


def per_device(n, ntp, wg, mg, sg, wu, mu, su, norm_train, norm_step):
    rows, columns = wg.shape
    length = norm_train.shape[0]
    lines = pl.cdiv(length, 128)
    as_lines = lambda x: jnp.pad(x, (0, lines * 128 - length)).reshape(lines, 128)
    wide = max(128, min(columns // 4, CHUNK // rows))
    height = min(rows // max(READS, SENDS), max(16, BODY // wide))
    chunks = columns // wide
    late = max(1, chunks * LATE // 8)
    main = chunks - late
    assert main > 0
    steps = 2 * main
    group = n * ntp
    f32, bf16 = jnp.float32, jnp.bfloat16
    dma = pltpu.SemaphoreType.DMA
    shapes = [
        ((rows, columns), f32),
        ((rows, columns), f32),
        ((n * rows, columns), bf16),
        ((n * rows, columns), bf16),
        ((columns // 128, 128), f32),
        ((columns // 128, 128), f32),
        ((group * lines, 128), bf16),
    ]
    between = list(shapes)
    between[2] = between[3] = ((n * rows, main * wide), bf16)
    between.append(((2 * late, rows + 8, wide), f32))
    anywhere = pl.BlockSpec(memory_space=pl.ANY)
    vmem = pl.BlockSpec(memory_space=pltpu.VMEM)
    latest_g, latest_u, ready_g, ready_u, scale_g, scale_u, norm, sent = pl.pallas_call(
        functools.partial(step_kernel, n, ntp, wide, height, late),
        out_shape=[pltpu.VMEM(shape, dtype) for shape, dtype in between],
        in_specs=[anywhere] * 6 + [pl.BlockSpec(memory_space=pltpu.HBM)] * 2,
        out_specs=[vmem] * len(between),
        scratch_shapes=[
            pltpu.VMEM((SLOTS, 3, rows, wide), f32),
            pltpu.VMEM((steps, n, 8, wide), f32),
            pltpu.VMEM((group, lines, 128), f32),
            pltpu.VMEM((2, lines, 128), f32),
            dma((SLOTS, READS)),
            dma,
            dma((n - 1,)),
            dma((RING, n - 1)),
            dma((2, n - 1)),
            dma((2, n - 1)),
            dma,
            dma,
        ],
        compiler_params=pltpu.CompilerParams(
            collective_id=0, has_side_effects=True, vmem_limit_bytes=14 << 20
        ),
        name="step",
    )(wg, mg, sg, wu, mu, su, *(pltpu.with_memory_space_constraint(as_lines(x), pltpu.HBM) for x in (norm_train, norm_step)))
    others = [lax.ppermute(sent, "zero", [(k, (k + d) % n) for k in range(n)]) for d in range(1, n)]
    costs = lambda size: pl.CostEstimate(flops=0, bytes_accessed=2 * size, transcendentals=0)
    as_out = lambda *k: [jax.ShapeDtypeStruct(*shapes[i]) for i in k]
    latest_g, latest_u, ready_g = pl.pallas_call(
        early_kernel,
        out_shape=as_out(0, 1, 2),
        in_specs=[vmem] * 3,
        out_specs=[anywhere] * 3,
        scratch_shapes=[dma((3,))],
        compiler_params=pltpu.CompilerParams(vmem_limit_bytes=1 << 20),
        cost_estimate=costs(12 * rows * columns),
        name="early",
    )(latest_g, latest_u, ready_g)
    ready_g, ready_u, scale_g, scale_u, norm = pl.pallas_call(
        functools.partial(rest_kernel, n, height),
        out_shape=as_out(2, 3, 4, 5, 6),
        in_specs=[vmem] * (5 + n - 1) + [anywhere],
        out_specs=[anywhere] * 5,
        input_output_aliases={5 + n - 1: 0},
        scratch_shapes=[
            pltpu.VMEM((2 * late, n * rows, wide), bf16),
            pltpu.VMEM((2, columns // 128, 128), f32),
            dma,
            dma((2 * late + 3,)),
        ],
        compiler_params=pltpu.CompilerParams(vmem_limit_bytes=6 << 20),
        cost_estimate=costs(4 * rows * columns),
        name="rest",
    )(ready_u, scale_g, scale_u, norm, sent, *others, ready_g)
    return (
        ready_g, ready_u, scale_g.reshape(columns), scale_u.reshape(columns),
        norm.reshape(group, lines * 128)[:, :length].reshape(group * length), latest_g, latest_u,
    )


def solution(mesh):
    block = P(("site", "zero"), "tp")
    return jax.shard_map(
        functools.partial(per_device, mesh.shape["zero"], mesh.shape["tp"]),
        mesh=mesh,
        in_specs=(block,) * 6 + (P(("site", "zero", "tp")),) * 2,
        out_specs=(
            P("site", "tp"), P("site", "tp"), P(("site", "tp")), P(("site", "tp")), P("site"), block, block,
        ),
        check_vma=False,
    )
```
